32 devices in a mesh: grp: 8 (over y, x, core), sp: 4 (over z).
Axes of the slice: x: 2, y: 2, z: 4, core: 2. Of those that a mesh axis runs over, the one named last changes fastest.
Arguments:
- latents: bfloat16 [8, 512, 3072], P('grp', 'sp'), may hold values from -6 to 6
- timestep: int32 [8], P('grp'), may hold values from 0 to 999
- w_mod: bfloat16 [256, 9216], replicated, may hold values from -0.375 to 0.375
- w_qkv: bfloat16 [4, 3072, 384], P('sp', 'grp'), may hold values from -2 to 2
- w_out: bfloat16 [4, 128, 3072], P('sp', 'grp'), may hold values from -0.5 to 0.5
Outputs:
- update: bfloat16 [8, 512, 3072], P('grp', 'sp')
The draws below stay inside these ranges and needn't reach their ends.
All inputs are finite; a program needn't handle non-finite values.
Results may differ from the reference program's by a relative error of at most 0.012.
Values may be sent and summed in bfloat16 or wider, within the bound.
A program may use at most 128 MiB of HBM per device.

```python
import math
import jax
import jax.numpy as jnp
from jax import lax

D = 3072
HS = 128
FREQ = 256
H = 4
LEN = 512
IMAGES = 8


def draw_w_qkv(key, part):
    first, second, third = jax.random.split(jax.random.fold_in(key, 17), 3)
    base = 1.0 / math.sqrt(D)
    query_part = jax.random.normal(first, (H, D, HS), jnp.float32) * (1.5 * base)
    value_part = jax.random.normal(third, (H, D, HS), jnp.float32) * base
    key_part = jax.random.normal(second, (H, D, HS), jnp.float32) * base
    whole = jnp.concatenate([query_part, key_part, value_part], axis=2)
    return jnp.clip(whole, -2.0, 2.0).astype(jnp.bfloat16)


def plant(array, stream_key, smallest, top_value):
    spot = [jax.random.randint(jax.random.fold_in(stream_key, axis), (), 0, length) for axis, length in enumerate(array.shape)]
    main_axis = array.shape.index(max(array.shape))
    next_to = spot[:main_axis] + [(spot[main_axis] + 1) % array.shape[main_axis]] + spot[main_axis + 1:]
    return array.at[tuple(spot)].set(smallest).at[tuple(next_to)].set(top_value)


def shard_levels(rng, shape, cuts, low, high):
    level, own = 1.0, jax.random.fold_in(rng, 6)
    for dim, shards_of in cuts:
        steps = jnp.exp(jax.random.uniform(jax.random.fold_in(own, dim), (shards_of,), jnp.float32, low / len(cuts), high / len(cuts)))
        level = level * jnp.repeat(steps, shape[dim] // shards_of).reshape([-1 if axis == dim else 1 for axis in range(len(shape))])
    return level


def centred(stream_key, shape, scale, limit, cuts=(), held_as=jnp.bfloat16):
    array = jax.random.normal(stream_key, shape, jnp.float32) * scale
    if len(cuts) > 0:
        array = shard_levels(stream_key, shape, cuts, -0.22, 0.18) * array
    return jnp.clip(array, min=-limit, max=limit).astype(held_as)


def setup_inputs(seed: int = 0) -> dict:
    arg_keys = jax.random.split(jax.random.key(seed), 6)
    latents = centred(arg_keys[0], (IMAGES, LEN, D), 1.0, 6.0, ((0, 8), (1, 4)))
    timestep = plant(jax.random.randint(arg_keys[1], (IMAGES,), 0, 1000), jax.random.fold_in(arg_keys[1], 1), 0, 999).astype(jnp.int32)
    w_mod = centred(arg_keys[2], (FREQ, 3 * D), FREQ ** -0.5, 0.375)
    w_qkv = draw_w_qkv(jax.random.fold_in(arg_keys[5], 71), 0)
    w_out = centred(arg_keys[4], (H, HS, D), HS ** -0.5, 0.5, ((0, 4), (1, 8)))
    return {"latents": latents, "timestep": timestep, "w_mod": w_mod, "w_qkv": w_qkv, "w_out": w_out}


def modulation(timestep, w_mod):
    half_freq = w_mod.shape[0] // 2
    freqs = jnp.exp(-math.log(10000.0) * jnp.arange(half_freq, dtype=jnp.float32) / half_freq)
    angles = timestep.astype(jnp.float32)[:, None] * freqs[None, :]
    embed = jnp.concatenate([jnp.cos(angles), jnp.sin(angles)], axis=1).astype(jnp.bfloat16)
    return jnp.dot(embed, w_mod, preferred_element_type=jnp.float32)

def normalize(latents, shift, scale):
    values = latents.astype(jnp.float32)
    center = lax.optimization_barrier(jnp.mean(values, axis=-1, keepdims=True))
    spread = lax.optimization_barrier(jnp.mean((values - center) ** 2, axis=-1, keepdims=True))
    normed = (values - center) * lax.rsqrt(spread + 1e-06)
    return (normed * (1.0 + scale[:, None, :]) + shift[:, None, :]).astype(jnp.bfloat16)

def attend(query, keys, values):
    length, head_size = query.shape
    block = min(512, length)
    blocks = query.reshape(length // block, block, head_size)

    def one_block(query_rows):
        scores = lax.dot_general(query_rows, keys, (((1,), (1,)), ((), ())), preferred_element_type=jnp.float32)
        scores = scores / math.sqrt(head_size)
        largest = lax.optimization_barrier(jnp.max(scores, axis=1, keepdims=True))
        weights = jnp.exp(scores - largest)
        probs = (weights / lax.optimization_barrier(jnp.sum(weights, axis=1, keepdims=True))).astype(jnp.bfloat16)
        return jnp.dot(probs, values, preferred_element_type=jnp.float32).astype(jnp.bfloat16)
    return lax.map(one_block, blocks).reshape(length, head_size)

def reference(latents, timestep, w_mod, w_qkv, w_out):
    width = latents.shape[2]
    head_size = w_out.shape[1]
    mod = modulation(timestep, w_mod)
    shift = mod[:, :width]
    scale = mod[:, width:2 * width]
    gate = mod[:, 2 * width:]
    normed = normalize(latents, shift, scale)

    def one_image(inputs):
        normed_one, gate_one = inputs

        def one_head(total, weights):
            weight_in, weight_out = weights
            qkv = jnp.dot(normed_one, weight_in, preferred_element_type=jnp.float32).astype(jnp.bfloat16)
            attended = attend(qkv[:, :head_size], qkv[:, head_size:2 * head_size], qkv[:, 2 * head_size:])
            contrib = jnp.dot(attended, weight_out, preferred_element_type=jnp.float32).astype(jnp.bfloat16)
            contrib = lax.optimization_barrier(contrib)
            return (total + contrib.astype(jnp.float32), None)
        start_total = jnp.zeros((normed_one.shape[0], width), jnp.float32)
        total, unused = lax.scan(one_head, start_total, (w_qkv, w_out))
        return (gate_one[None, :] * total).astype(jnp.bfloat16)
    return lax.map(one_image, (normed, gate))
```

```python
import functools
import math

import jax
import jax.numpy as jnp
from jax import lax
from jax.experimental import pallas as pl
from jax.experimental.pallas import tpu as pltpu
from jax.sharding import PartitionSpec as P

MESH = pl.DeviceIdType.MESH
CHUNKS = 4
LIMIT = 40 * 2**20


def embedding(timestep, freq):
    half_freq = freq // 2
    steps = lax.broadcasted_iota(jnp.int32, (8, half_freq), 1).astype(jnp.float32)
    angles = timestep.astype(jnp.float32) * jnp.exp(-math.log(10000.0) * steps / half_freq)
    return jnp.concatenate([jnp.cos(angles), jnp.sin(angles)], axis=1).astype(jnp.bfloat16)


def kernel(
    n_grp,
    n_sp,
    step_now,
    lat_hbm,
    wmod_hbm,
    wqkv_hbm,
    wout_hbm,
    att_mine,
    wo,
    mod,
    lat,
    wmod,
    normed,
    wq,
    q_buf,
    kv,
    att_send,
    loc_sem,
    q_s,
    o_s,
    lat_s,
    kv_s,
    at_s,
    wz_r,
    wx_r,
    wd_r,
    oz_r,
    ox_r,
    od_r,
    lat_r,
    kv_r,
    at_r,
):
    g = lax.axis_index("grp")
    s = lax.axis_index("sp")
    core, chip = g % 2, g // 2
    chips = n_grp // 2
    pairs = n_sp // 2
    parity, pair = s % 2, s // 2
    tok, width = lat_hbm.shape[1], lat_hbm.shape[2]
    rows_q = wqkv_hbm.shape[1]
    rows_o = wout_hbm.shape[1]
    head = wqkv_hbm.shape[2] // 3
    sib = (chip * 2 + 1 - core, s)
    mate = (g, pair * 2 + 1 - parity)

    def at_chip(c):
        return ((chip + c) % chips * 2 + core, s)

    def at_pair(k, flip):
        return (g, (pair + k) % pairs * 2 + (parity + flip) % 2)

    def remote(src, dst, ssem, rsem, device):
        return pltpu.make_async_remote_copy(
            src_ref=src, dst_ref=dst, send_sem=ssem, recv_sem=rsem, device_id=device, device_id_type=MESH
        )

    def wq_rows(k, owner):
        return wq.at[pl.ds(pl.multiple_of(k * width + owner * rows_q, rows_q), rows_q), :]

    def wo_rows(par, k, owner):
        first = (par * pairs + k) * head + owner * rows_o
        return wo.at[pl.ds(pl.multiple_of(first, rows_o), rows_o), :]

    barrier = pltpu.get_barrier_semaphore()
    peers = [sib] + [at_chip(c) for c in range(1, chips)]
    peers += [at_pair(k, f) for k in range(pairs) for f in range(2) if (k, f) != (0, 0)]
    for peer in peers:
        pl.semaphore_signal(barrier, inc=1, device_id=peer, device_id_type=MESH)
    local = [
        pltpu.make_async_copy(wqkv_hbm.at[0], wq_rows(0, g), loc_sem.at[0]),
        pltpu.make_async_copy(wout_hbm.at[0], wo_rows(parity, 0, g), loc_sem.at[1]),
        pltpu.make_async_copy(lat_hbm.at[0], lat.at[0], loc_sem.at[2]),
        pltpu.make_async_copy(wmod_hbm, wmod, loc_sem.at[3]),
    ]
    for copy in local:
        copy.start()
    local[0].wait()
    local[1].wait()
    local[2].wait()
    pl.semaphore_wait(barrier, len(peers))

    sent = {"q": 0, "o": 0}

    def start(src, dst, ssem, rsem, device, kind=None):
        remote(src, dst, ssem, rsem, device).start()
        if kind is not None:
            sent[kind] += math.prod(src.shape)

    def arrive(region, ssem, rsem):
        remote(region, region, ssem, rsem, sib).wait_recv()

    square = chips == 4
    near_x = chip // 2 * 2 + 1 - chip % 2
    near_y = (chip + 2) % 4
    corner = (near_x + 2) % 4
    to_x, to_y = (near_x * 2 + core, s), (near_y * 2 + core, s)
    others = [near_x, near_y, corner] if square else [(chip + chips - c) % chips for c in range(1, chips)]

    def q_part(k, owner, half):
        size = rows_q // 2
        return wq.at[pl.ds(pl.multiple_of(k * width + owner * rows_q + half * size, size), size), :]

    def o_part(par, k, owner, half):
        first = (par * pairs + k) * head + owner * rows_o
        size = width // 2
        return wo.at[pl.ds(pl.multiple_of(first, rows_o), rows_o), half * size : (half + 1) * size]

    class Spread:
        def __init__(self, kind, i, whole, part, ssem, xr, dr):
            self.kind, self.i, self.whole, self.part = kind, i, whole, part
            self.ssem, self.xr, self.dr = ssem, xr, dr

        def cross(self, region, slot, device):
            start(region, region, self.ssem, self.xr.at[self.i, slot], device, self.kind)

        def land(self, region, slot):
            arrive(region, self.ssem, self.xr.at[self.i, slot])

        def to_sib(self, region):
            start(region, region, self.ssem, self.dr, sib, self.kind)

        def begin(self):
            mine = self.whole(g)
            if square:
                self.cross(mine, 0, to_x)
                self.cross(mine, 1, to_y)
            else:
                for c in range(1, chips):
                    self.cross(mine, c - 1, at_chip(c))
            self.to_sib(mine)

        def relay(self):
            if square:
                for slot, device in ((0, to_y), (1, to_x)):
                    owner = others[slot] * 2 + core
                    self.land(self.whole(owner), slot)
                    self.cross(self.part(owner, slot), 2 + slot, device)
                    self.to_sib(self.whole(owner))
            else:
                for slot in range(chips - 1):
                    region = self.whole(others[slot] * 2 + core)
                    self.land(region, slot)
                    self.to_sib(region)

        def last(self):
            if square:
                owner = corner * 2 + core
                self.land(self.part(owner, 0), 2)
                self.land(self.part(owner, 1), 3)
                self.to_sib(self.whole(owner))

    def spread_q(k):
        whole, part = functools.partial(wq_rows, k), functools.partial(q_part, k)
        return Spread("q", k, whole, part, q_s, wx_r, wd_r.at[k])

    def finish_q(k):
        arrive(wq.at[k * width : k * width + width // 2, :], q_s, wd_r.at[k])

    def spread_o(k, flip):
        par = (parity + flip) % 2
        whole, part = functools.partial(wo_rows, par, k), functools.partial(o_part, par, k)
        return Spread("o", k * 2 + flip, whole, part, o_s, ox_r, od_r)

    far = [(k, f) for k in range(pairs) for f in range(2) if (k, f) != (0, 0)]
    all_q = [spread_q(k) for k in range(pairs)]
    near_o, far_o = spread_o(0, 0), [spread_o(k, f) for k, f in far]

    def land_o(n):
        k, f = far[n]
        i = k * 2 + f
        arrive(wo_rows((parity + f) % 2, k, g), o_s, oz_r.at[i])
        far_o[n].begin()

    all_q[0].begin()
    for k in range(1, pairs):
        start(wq_rows(0, g), wq_rows(k, g), q_s, wz_r.at[k], at_pair(k, 0), "q")

    def send_o(n):
        for k, f in far[n : n + 1]:
            i = k * 2 + f
            start(wo_rows(parity, 0, g), wo_rows(parity, k, g), o_s, oz_r.at[i], at_pair(k, f), "o")

    piece = tok // CHUNKS

    def send_chunk(c):
        rows = pl.ds(c * piece, piece)
        start(lat.at[0, rows, :], lat.at[1, rows, :], lat_s, lat_r.at[c], mate)

    send_chunk(0)

    embed = embedding(step_now[0], wmod.shape[0])
    embed = jnp.concatenate([embed, embed], axis=0)
    local[3].wait()
    step = min(512, width)

    @pl.loop(0, 3 * width // step)
    def _(i):
        cols = pl.ds(pl.multiple_of(i * step, step), step)
        part = jnp.dot(embed, wmod[:, cols], preferred_element_type=jnp.float32)
        mod[:, cols] = part[:8]

    def normalize(which, first, count):
        block = 16

        @pl.loop(0, count // block)
        def _(i):
            rows = pl.ds(pl.multiple_of(first + i * block, block), block)
            values = lat[which, rows, :].astype(jnp.float32)
            center = jnp.mean(values, axis=-1, keepdims=True)
            values = values - center
            spread = jnp.mean(values * values, axis=-1, keepdims=True)
            scaled = values * lax.rsqrt(spread + 1e-06)
            shift = mod[0:1, 0:width]
            scale = mod[0:1, width : 2 * width]
            target = pl.ds(pl.multiple_of(which * tok + first + i * block, block), block)
            normed[target, :] = (scaled * (1.0 + scale) + shift).astype(jnp.bfloat16)

    def normalize_chunk(c):
        region = lat.at[1, pl.ds(c * piece, piece), :]
        arrive(region, lat_s, lat_r.at[c])
        normalize(1, c * piece, piece)

    spans = [(0, tok), (tok, tok - piece), (2 * tok - piece, piece)]

    def project(k, part):
        rows = pl.ds(*spans[part])
        result = jnp.dot(normed[rows, :], wq[k * width : (k + 1) * width, :], preferred_element_type=jnp.float32).astype(jnp.bfloat16)
        q_buf[k, rows, :] = result[:, :head]
        kv[0, k, rows, :] = result[:, head:]

    def share_kv(k, part):
        rows = pl.ds(*spans[part])
        for d in range(1, pairs):
            there = (k + d) % pairs
            start(kv.at[0, k, rows, :], kv.at[d, there, rows, :], kv_s, kv_r.at[d - 1, there], at_pair(d, 0))

    normalize(0, 0, tok)
    all_q[0].relay()
    near_o.begin()
    send_chunk(1)
    for k in range(1, pairs):
        arrive(wq_rows(k, g), q_s, wz_r.at[k])
        all_q[k].begin()
    send_o(0)
    send_chunk(2)
    send_o(1)
    send_chunk(3)
    for n in range(2, len(far)):
        send_o(n)
    all_q[0].last()
    near_o.relay()
    finish_q(0)
    project(0, 0)
    share_kv(0, 0)
    near_o.last()
    for k in range(1, pairs):
        all_q[k].relay()
    normalize_chunk(0)
    for k in range(1, pairs):
        all_q[k].last()
        finish_q(k)
        project(k, 0)
        share_kv(k, 0)
    land_o(0)
    land_o(1)
    for c in range(1, CHUNKS - 1):
        normalize_chunk(c)
    for k in range(pairs):
        project(k, 1)
        share_kv(k, 1)
    normalize_chunk(CHUNKS - 1)
    for k in range(pairs):
        project(k, 2)
        share_kv(k, 2)
    far_o[0].relay()
    for n in range(2, len(far)):
        land_o(n)
    far_o[1].relay()
    far_o[0].last()

    def attend(k):
        for d in range(1, pairs):
            arrive(kv.at[d, k], kv_s, kv_r.at[d - 1, k])
        total = pairs * 2 * tok
        keys = kv[:, k, :, :head].reshape(total, head)
        values = kv[:, k, :, head:].reshape(total, head)
        cols = pl.ds(pl.multiple_of((parity * pairs + k) * head, head), head)
        for which in (1, 0):
            query = q_buf[k, pl.ds(which * tok, tok), :]
            scores = lax.dot_general(query, keys, (((1,), (1,)), ((), ())), preferred_element_type=jnp.float32)
            scores = scores / math.sqrt(head)
            largest = jnp.max(scores, axis=1, keepdims=True)
            weights = jnp.exp(scores - largest)
            probs = (weights / jnp.sum(weights, axis=1, keepdims=True)).astype(jnp.bfloat16)
            result = jnp.dot(probs, values, preferred_element_type=jnp.float32).astype(jnp.bfloat16)
            if which == 1:
                att_send[k] = result
                start(att_send.at[k], att_mine.at[:, cols], at_s, at_r, mate)
            else:
                att_mine[:, cols] = result

    attend(0)
    for spread in far_o[2:]:
        spread.relay()
    far_o[1].last()
    for k in range(1, pairs):
        attend(k)
    for spread in far_o[2:]:
        spread.last()
    arrive(wo.at[0 : n_sp * head // 2, :], o_s, od_r)
    arrive(att_send, at_s, at_r)

    def drain(region, ssem):
        remote(region, region, ssem, at_r, sib).wait_send()

    drain(wq.at[0 : sent["q"] // wq.shape[1], :], q_s)
    drain(wo.at[0 : sent["o"] // width, :], o_s)
    drain(lat.at[0], lat_s)
    for d in range(1, pairs):
        drain(kv.at[0], kv_s)
    drain(att_send, at_s)


def project_out(att, wo, mod, out_hbm, out_buf, sems):
    width = wo.shape[1]
    step = width // sems.shape[0]
    outs = []
    for i in range(sems.shape[0]):
        cols = slice(i * step, (i + 1) * step)
        total = jnp.dot(att[...], wo[:, cols], preferred_element_type=jnp.float32)
        gate = mod[0:1, 2 * width + i * step : 2 * width + (i + 1) * step]
        out_buf[:, cols] = (gate * total).astype(jnp.bfloat16)
        outs.append(pltpu.make_async_copy(out_buf.at[:, cols], out_hbm.at[0, :, cols], sems.at[i]))
        outs[i].start()
    for copy in outs:
        copy.wait()


def on_device(n_grp, n_sp, latents, timestep, w_mod, w_qkv, w_out):
    _, tok, width = latents.shape
    head = w_qkv.shape[2] // 3
    pairs, chips = n_sp // 2, n_grp // 2
    dma = pltpu.SemaphoreType.DMA
    bf16 = jnp.bfloat16
    anywhere = pl.BlockSpec(memory_space=pl.ANY)
    vmem = pl.BlockSpec(memory_space=pltpu.VMEM)
    args = [pltpu.with_memory_space_constraint(a, pltpu.HBM) for a in (latents, w_mod, w_qkv, w_out)]
    att, wo, mod = pl.pallas_call(
        functools.partial(kernel, n_grp, n_sp),
        out_shape=[
            pltpu.VMEM((tok, n_sp * head), bf16),
            pltpu.VMEM((n_sp * head, width), bf16),
            pltpu.VMEM((8, w_mod.shape[1]), jnp.float32),
        ],
        in_specs=[pl.BlockSpec(memory_space=pltpu.SMEM)] + [anywhere] * 4,
        out_specs=[vmem] * 3,
        scratch_shapes=[
            pltpu.VMEM((2, tok, width), bf16),
            pltpu.VMEM(w_mod.shape, bf16),
            pltpu.VMEM((2 * tok, width), bf16),
            pltpu.VMEM((pairs * width, 3 * head), bf16),
            pltpu.VMEM((pairs, 2 * tok, head), bf16),
            pltpu.VMEM((pairs, pairs, 2 * tok, 2 * head), bf16),
            pltpu.VMEM((pairs, tok, head), bf16),
            dma((4,)),
            dma,
            dma,
            dma,
            dma,
            dma,
            dma((pairs,)),
            dma((pairs, max(chips - 1, 4))),
            dma((pairs,)),
            dma((n_sp,)),
            dma((n_sp, max(chips - 1, 4))),
            dma,
            dma((CHUNKS,)),
            dma((max(pairs - 1, 1), pairs)),
            dma,
        ],
        compiler_params=pltpu.CompilerParams(collective_id=0, has_side_effects=True, vmem_limit_bytes=LIMIT),
    )(timestep, *args)
    return pl.pallas_call(
        project_out,
        out_shape=jax.ShapeDtypeStruct(latents.shape, bf16),
        in_specs=[vmem] * 3,
        out_specs=anywhere,
        scratch_shapes=[pltpu.VMEM((tok, width), bf16), dma((max(width // 512, 1),))],
        compiler_params=pltpu.CompilerParams(vmem_limit_bytes=8 * 2**20),
    )(att, wo, mod)


def solution(mesh):
    placed = (P("grp", "sp", None), P("grp"), P(), P("sp", "grp", None), P("sp", "grp", None))
    body = functools.partial(on_device, mesh.shape["grp"], mesh.shape["sp"])
    return jax.shard_map(
        body, mesh=mesh, in_specs=placed, out_specs=P("grp", "sp", None), check_vma=False
    )
```

```python
import functools
import math

import jax
import jax.numpy as jnp
from jax import lax
from jax.experimental import pallas as pl
from jax.experimental.pallas import tpu as pltpu
from jax.sharding import PartitionSpec as P

MESH = pl.DeviceIdType.MESH
CHUNKS = 4
LIMIT = 40 * 2**20


def embedding(timestep, freq):
    half_freq = freq // 2
    steps = lax.broadcasted_iota(jnp.int32, (8, half_freq), 1).astype(jnp.float32)
    angles = timestep.astype(jnp.float32) * jnp.exp(-math.log(10000.0) * steps / half_freq)
    return jnp.concatenate([jnp.cos(angles), jnp.sin(angles)], axis=1).astype(jnp.bfloat16)


def kernel(
    n_grp,
    n_sp,
    step_now,
    lat_hbm,
    wmod_hbm,
    wqkv_hbm,
    wout_hbm,
    att_mine,
    wo,
    mod,
    lat,
    wmod,
    normed,
    wq,
    q_buf,
    kv,
    att_send,
    att_far,
    loc_sem,
    q_s,
    o_s,
    lat_s,
    kv_s,
    at_s,
    wz_r,
    wx_r,
    wd_r,
    oz_r,
    ox_r,
    od_r,
    lat_r,
    kv_r,
    at_r,
    x_r,
):
    g = lax.axis_index("grp")
    s = lax.axis_index("sp")
    core, chip = g % 2, g // 2
    chips = n_grp // 2
    pairs = n_sp // 2
    parity, pair = s % 2, s // 2
    tok, width = lat_hbm.shape[1], lat_hbm.shape[2]
    rows_q = wqkv_hbm.shape[1]
    rows_o = wout_hbm.shape[1]
    head = wqkv_hbm.shape[2] // 3
    sib = (chip * 2 + 1 - core, s)
    mate = (g, pair * 2 + 1 - parity)
    line = n_sp == 4
    inner = (parity + pair) % 2
    piece = tok // CHUNKS
    part_rows = tok - piece

    def at_chip(c):
        return ((chip + c) % chips * 2 + core, s)

    def at_pair(k, flip):
        return (g, (pair + k) % pairs * 2 + (parity + flip) % 2)

    def when_inner(body):
        pl.when(inner == 1)(body)

    def when_outer(body):
        pl.when(inner == 0)(body)

    def remote(src, dst, ssem, rsem, device):
        return pltpu.make_async_remote_copy(
            src_ref=src, dst_ref=dst, send_sem=ssem, recv_sem=rsem, device_id=device, device_id_type=MESH
        )

    def wq_rows(k, owner):
        return wq.at[pl.ds(pl.multiple_of(k * width + owner * rows_q, rows_q), rows_q), :]

    def wo_rows(par, k, owner):
        first = (par * pairs + k) * head + owner * rows_o
        return wo.at[pl.ds(pl.multiple_of(first, rows_o), rows_o), :]

    barrier = pltpu.get_barrier_semaphore()
    peers = [sib] + [at_chip(c) for c in range(1, chips)]
    peers += [at_pair(k, f) for k in range(pairs) for f in range(2) if (k, f) != (0, 0)]
    for peer in peers:
        pl.semaphore_signal(barrier, inc=1, device_id=peer, device_id_type=MESH)
    local = [
        pltpu.make_async_copy(wqkv_hbm.at[0], wq_rows(0, g), loc_sem.at[0]),
        pltpu.make_async_copy(wout_hbm.at[0], wo_rows(parity, 0, g), loc_sem.at[1]),
        pltpu.make_async_copy(lat_hbm.at[0], lat.at[0:tok, :], loc_sem.at[2]),
        pltpu.make_async_copy(wmod_hbm, wmod, loc_sem.at[3]),
    ]
    for copy in local:
        copy.start()
    local[0].wait()
    local[1].wait()
    local[2].wait()
    pl.semaphore_wait(barrier, len(peers))

    def start(src, dst, ssem, rsem, device):
        remote(src, dst, ssem, rsem, device).start()

    def arrive(region, ssem, rsem):
        remote(region, region, ssem, rsem, sib).wait_recv()

    square = chips == 4
    near_x = chip // 2 * 2 + 1 - chip % 2
    near_y = (chip + 2) % 4
    corner = (near_x + 2) % 4
    to_x, to_y = (near_x * 2 + core, s), (near_y * 2 + core, s)
    others = [near_x, near_y, corner] if square else [(chip + chips - c) % chips for c in range(1, chips)]

    def q_part(k, owner, half):
        size = rows_q // 2
        return wq.at[pl.ds(pl.multiple_of(k * width + owner * rows_q + half * size, size), size), :]

    def o_part(par, k, owner, half):
        first = (par * pairs + k) * head + owner * rows_o
        size = width // 2
        return wo.at[pl.ds(pl.multiple_of(first, rows_o), rows_o), half * size : (half + 1) * size]

    class Spread:
        def __init__(self, i, whole, part, ssem, xr, dr):
            self.i, self.whole, self.part = i, whole, part
            self.ssem, self.xr, self.dr = ssem, xr, dr

        def cross(self, region, slot, device):
            start(region, region, self.ssem, self.xr.at[self.i, slot], device)

        def land(self, region, slot):
            arrive(region, self.ssem, self.xr.at[self.i, slot])

        def to_sib(self, region):
            start(region, region, self.ssem, self.dr, sib)

        def begin(self):
            mine = self.whole(g)
            if square:
                self.cross(mine, 0, to_x)
                self.cross(mine, 1, to_y)
            else:
                for c in range(1, chips):
                    self.cross(mine, c - 1, at_chip(c))
            self.to_sib(mine)

        def relay(self):
            if square:
                for slot, device in ((0, to_y), (1, to_x)):
                    owner = others[slot] * 2 + core
                    self.land(self.whole(owner), slot)
                    self.cross(self.part(owner, slot), 2 + slot, device)
                    self.to_sib(self.whole(owner))
            else:
                for slot in range(chips - 1):
                    region = self.whole(others[slot] * 2 + core)
                    self.land(region, slot)
                    self.to_sib(region)

        def last(self):
            if square:
                owner = corner * 2 + core
                self.land(self.part(owner, 0), 2)
                self.land(self.part(owner, 1), 3)
                self.to_sib(self.whole(owner))

    def spread_q(k):
        whole, part = functools.partial(wq_rows, k), functools.partial(q_part, k)
        return Spread(k, whole, part, q_s, wx_r, wd_r.at[k])

    def finish_q(k):
        arrive(wq.at[k * width : k * width + width // 2, :], q_s, wd_r.at[k])

    def spread_o(k, flip):
        par = (parity + flip) % 2
        whole, part = functools.partial(wo_rows, par, k), functools.partial(o_part, par, k)
        return Spread(k * 2 + flip, whole, part, o_s, ox_r, od_r)

    far = [(k, f) for k in range(pairs) for f in range(2) if (k, f) != (0, 0)]
    all_q = [spread_q(k) for k in range(pairs)]
    near_o = spread_o(0, 0)

    def send_q():
        for k in range(1, pairs):
            start(wq_rows(0, g), wq_rows(k, g), q_s, wz_r.at[k], at_pair(k, 0))

    def pass_o(par, k_here, k_there, flip_there, device):
        start(wo_rows(par, k_here, g), wo_rows(par, k_there, g), o_s, oz_r.at[k_there * 2 + flip_there], device)

    def land_o(k, flip):
        arrive(wo_rows((parity + flip) % 2, k, g), o_s, oz_r.at[k * 2 + flip])

    def send_chunk(c):
        rows = c * piece
        start(lat.at[pl.ds(rows, piece), :], lat.at[pl.ds(tok + rows, piece), :], lat_s, lat_r.at[c], mate)

    def send_inner():
        start(lat.at[pl.ds(part_rows, piece), :], lat.at[pl.ds(2 * tok, piece), :], lat_s, x_r.at[0], at_pair(1, 1))

    step = min(512, width)

    def modulate():
        embed = embedding(step_now[0], wmod.shape[0])
        embed = jnp.concatenate([embed, embed], axis=0)
        local[3].wait()

        @pl.loop(0, 3 * width // step)
        def _(i):
            cols = pl.ds(pl.multiple_of(i * step, step), step)
            part = jnp.dot(embed, wmod[:, cols], preferred_element_type=jnp.float32)
            mod[:, cols] = part[:8]

    def normalize(first, count):
        block = 16

        @pl.loop(0, count // block)
        def _(i):
            rows = pl.ds(pl.multiple_of(first + i * block, block), block)
            values = lat[rows, :].astype(jnp.float32)
            center = jnp.mean(values, axis=-1, keepdims=True)
            values = values - center
            spread = jnp.mean(values * values, axis=-1, keepdims=True)
            scaled = values * lax.rsqrt(spread + 1e-06)
            shift = mod[0:1, 0:width]
            scale = mod[0:1, width : 2 * width]
            normed[rows, :] = (scaled * (1.0 + scale) + shift).astype(jnp.bfloat16)

    def land_chunk(c):
        arrive(lat.at[pl.ds(tok + c * piece, piece), :], lat_s, lat_r.at[c])

    def normalize_chunk(c):
        land_chunk(c)
        normalize(tok + c * piece, piece)

    def project(k, first, count):
        rows = pl.ds(first, count)
        weights = wq[k * width : (k + 1) * width, :]
        result = jnp.dot(normed[rows, :], weights, preferred_element_type=jnp.float32).astype(jnp.bfloat16)
        q_buf[k, rows, :] = result[:, :head]
        here = min(2 * tok - first, count)
        kv[0, k, pl.ds(first, here), :] = result[:here, head:]
        if here < count:
            kv[1, k, pl.ds(2 * tok - (count - here), count - here), :] = result[here:, head:]

    def share_kv(k, first, count):
        rows = pl.ds(first, count)
        for d in range(1, pairs):
            there = (k + d) % pairs
            start(kv.at[0, k, rows, :], kv.at[d, there, rows, :], kv_s, kv_r.at[d - 1, there], at_pair(d, 0))

    def attention(k, first, count):
        total = pairs * 2 * tok
        keys = kv[:, k, :, :head].reshape(total, head)
        values = kv[:, k, :, head:].reshape(total, head)
        query = q_buf[k, pl.ds(first, count), :]
        scores = lax.dot_general(query, keys, (((1,), (1,)), ((), ())), preferred_element_type=jnp.float32)
        scores = scores / math.sqrt(head)
        largest = jnp.max(scores, axis=1, keepdims=True)
        weights = jnp.exp(scores - largest)
        probs = (weights / jnp.sum(weights, axis=1, keepdims=True)).astype(jnp.bfloat16)
        return jnp.dot(probs, values, preferred_element_type=jnp.float32).astype(jnp.bfloat16)

    def att_cols(k):
        return pl.ds(pl.multiple_of((parity * pairs + k) * head, head), head)

    def send_att(k, count):
        rows = pl.ds(0, count)
        start(att_send.at[k, rows, :], att_mine.at[rows, att_cols(k)], at_s, at_r, mate)

    def drain(region, ssem):
        remote(region, region, ssem, at_r, sib).wait_send()

    spread_sends = 7 if square else 2 * chips - 1

    def drain_o(passed):
        drain(wq.at[0 : (n_sp * spread_sends + passed) * rows_o * width // (3 * head), :], o_s)

    def general():
        far_o = [spread_o(k, f) for k, f in far]

        def send_o(n):
            for k, f in far[n : n + 1]:
                pass_o(parity, 0, k, f, at_pair(k, f))

        def take_o(n):
            land_o(*far[n])
            far_o[n].begin()

        all_q[0].begin()
        near_o.begin()
        send_q()
        send_chunk(0)
        modulate()
        normalize(0, tok)
        all_q[0].relay()
        near_o.relay()
        send_chunk(1)
        for k in range(1, pairs):
            arrive(wq_rows(k, g), q_s, wz_r.at[k])
            all_q[k].begin()
        send_o(0)
        send_chunk(2)
        send_o(1)
        send_chunk(3)
        for n in range(2, len(far)):
            send_o(n)
        all_q[0].last()
        finish_q(0)
        project(0, 0, tok)
        share_kv(0, 0, tok)
        near_o.last()
        for k in range(1, pairs):
            all_q[k].relay()
        normalize_chunk(0)
        for k in range(1, pairs):
            all_q[k].last()
            finish_q(k)
            project(k, 0, tok)
            share_kv(k, 0, tok)
        take_o(0)
        take_o(1)
        for c in range(1, CHUNKS):
            normalize_chunk(c)
        for k in range(pairs):
            project(k, tok, tok)
            share_kv(k, tok, tok)
        far_o[0].relay()
        for n in range(2, len(far)):
            take_o(n)
        far_o[1].relay()
        far_o[0].last()
        for spread in far_o[2:]:
            spread.relay()
        far_o[1].last()
        for k in range(pairs):
            for d in range(1, pairs):
                arrive(kv.at[d, k], kv_s, kv_r.at[d - 1, k])
            att_send[k] = attention(k, tok, tok)
            send_att(k, tok)
            att_mine[:, att_cols(k)] = attention(k, 0, tok)
        for spread in far_o[2:]:
            spread.last()
        arrive(wo.at[0 : n_sp * head // 2, :], o_s, od_r)
        arrive(att_send, at_s, at_r)
        drain_o(n_sp - 1)
        for d in range(1, pairs):
            drain(kv.at[0], kv_s)
        drain(att_send, at_s)

    def along_line():
        far_a, far_b, far_c = spread_o(0, 1), spread_o(1, inner), spread_o(1, 1 - inner)
        all_q[0].begin()
        near_o.begin()
        send_q()
        send_chunk(0)

        @when_outer
        def _():
            pass_o(parity, 0, 0, 1, mate)
            for c in range(1, CHUNKS):
                send_chunk(c)

        modulate()
        normalize(0, tok)

        @when_inner
        def _():
            pass_o(parity, 0, 0, 1, mate)
            pass_o(parity, 0, 1, 1, at_pair(1, 1))

        all_q[0].relay()
        near_o.relay()
        arrive(wq_rows(1, g), q_s, wz_r.at[1])
        all_q[1].begin()

        @when_inner
        def _():
            for c in range(1, CHUNKS - 1):
                send_chunk(c)
            send_inner()

        normalize_chunk(0)
        all_q[0].last()
        finish_q(0)
        project(0, 0, tok)
        share_kv(0, 0, tok)
        near_o.last()
        land_o(0, 1)

        @when_inner
        def _():
            pass_o(1 - parity, 0, 1, 0, at_pair(1, 1))

        far_a.begin()
        normalize_chunk(1)

        @when_inner
        def _():
            land_o(1, 1)
            pass_o(1 - parity, 1, 1, 0, mate)
            land_o(1, 0)
            pass_o(parity, 1, 1, 1, mate)

        all_q[1].relay()
        far_a.relay()

        @when_inner
        def _():
            far_b.begin()
            far_c.begin()

        all_q[1].last()
        finish_q(1)
        project(1, 0, tok)
        share_kv(1, 0, tok)
        far_a.last()
        normalize_chunk(2)

        @when_outer
        def _():
            land_o(1, 0)
            far_b.begin()

        for k in range(pairs):
            project(k, tok, part_rows)
            share_kv(k, tok, part_rows)

        @when_outer
        def _():
            land_o(1, 1)
            far_c.begin()

        @when_inner
        def _():
            far_b.relay()
            land_chunk(CHUNKS - 1)
            arrive(lat.at[pl.ds(2 * tok, piece), :], lat_s, x_r.at[0])
            normalize(2 * tok - piece, 2 * piece)
            rows = pl.ds(2 * tok - piece, piece)
            for k in range(pairs):
                project(k, 2 * tok - piece, 2 * piece)
                start(kv.at[1, k, rows, :], kv.at[0, 1 - k, rows, :], kv_s, x_r.at[2 - k], at_pair(1, 0))
                share_kv(k, 2 * tok - piece, piece)

        @when_outer
        def _():
            far_b.relay()

        far_c.relay()
        far_b.last()
        far_c.last()
        for k in range(pairs):

            @when_inner
            def _():
                arrive(kv.at[1, k, pl.ds(0, tok + part_rows), :], kv_s, kv_r.at[0, k])
                there = pl.ds(pl.multiple_of((parity * pairs + 1 - k) * head, head), head)
                far_rows = pl.ds(part_rows, piece)
                att_send[k] = attention(k, tok, tok)
                send_att(k, tok)
                att_far[k] = attention(k, 2 * tok, piece)
                start(att_far.at[k], att_mine.at[far_rows, there], at_s, x_r.at[3], at_pair(1, 1))

            @when_outer
            def _():
                arrive(kv.at[1, k], kv_s, kv_r.at[0, k])
                arrive(kv.at[0, k, pl.ds(2 * tok - piece, piece), :], kv_s, x_r.at[1 + k])
                att_send[k, 0:part_rows] = attention(k, tok, part_rows)
                send_att(k, part_rows)

            att_mine[:, att_cols(k)] = attention(k, 0, tok)
        arrive(wo.at[0 : n_sp * head // 2, :], o_s, od_r)

        @when_inner
        def _():
            arrive(att_send.at[:, pl.ds(0, part_rows), :], at_s, at_r)
            arrive(att_far, at_s, x_r.at[3])
            drain_o(5)
            drain(lat.at[0 : pairs * (2 * tok + piece) * 2 * head // width, :], kv_s)
            drain(q_buf.at[:, pl.ds(0, tok + piece), :], at_s)

        @when_outer
        def _():
            arrive(att_send, at_s, at_r)
            drain_o(1)
            drain(kv.at[0, :, pl.ds(0, tok + part_rows), :], kv_s)
            drain(att_send.at[:, pl.ds(0, part_rows), :], at_s)

    if line:
        along_line()
    else:
        general()
    drain(wq.at[0 : (pairs * spread_sends + pairs - 1) * rows_q, :], q_s)
    drain(lat.at[0:tok, :], lat_s)


def project_out(att, wo, mod, out_hbm, out_buf, sems):
    width = wo.shape[1]
    step = width // sems.shape[0]
    outs = []
    for i in range(sems.shape[0]):
        cols = slice(i * step, (i + 1) * step)
        total = jnp.dot(att[...], wo[:, cols], preferred_element_type=jnp.float32)
        gate = mod[0:1, 2 * width + i * step : 2 * width + (i + 1) * step]
        out_buf[:, cols] = (gate * total).astype(jnp.bfloat16)
        outs.append(pltpu.make_async_copy(out_buf.at[:, cols], out_hbm.at[0, :, cols], sems.at[i]))
        outs[i].start()
    for copy in outs:
        copy.wait()


def on_device(n_grp, n_sp, latents, timestep, w_mod, w_qkv, w_out):
    _, tok, width = latents.shape
    head = w_qkv.shape[2] // 3
    pairs, chips = n_sp // 2, n_grp // 2
    dma = pltpu.SemaphoreType.DMA
    bf16 = jnp.bfloat16
    anywhere = pl.BlockSpec(memory_space=pl.ANY)
    vmem = pl.BlockSpec(memory_space=pltpu.VMEM)
    args = [pltpu.with_memory_space_constraint(a, pltpu.HBM) for a in (latents, w_mod, w_qkv, w_out)]
    att, wo, mod = pl.pallas_call(
        functools.partial(kernel, n_grp, n_sp),
        out_shape=[
            pltpu.VMEM((tok, n_sp * head), bf16),
            pltpu.VMEM((n_sp * head, width), bf16),
            pltpu.VMEM((8, w_mod.shape[1]), jnp.float32),
        ],
        in_specs=[pl.BlockSpec(memory_space=pltpu.SMEM)] + [anywhere] * 4,
        out_specs=[vmem] * 3,
        scratch_shapes=[
            pltpu.VMEM((2 * tok + tok // CHUNKS, width), bf16),
            pltpu.VMEM(w_mod.shape, bf16),
            pltpu.VMEM((2 * tok + tok // CHUNKS, width), bf16),
            pltpu.VMEM((pairs * width, 3 * head), bf16),
            pltpu.VMEM((pairs, 2 * tok + tok // CHUNKS, head), bf16),
            pltpu.VMEM((pairs, pairs, 2 * tok, 2 * head), bf16),
            pltpu.VMEM((pairs, tok, head), bf16),
            pltpu.VMEM((pairs, tok // CHUNKS, head), bf16),
            dma((4,)),
            dma,
            dma,
            dma,
            dma,
            dma,
            dma((pairs,)),
            dma((pairs, max(chips - 1, 4))),
            dma((pairs,)),
            dma((n_sp,)),
            dma((n_sp, max(chips - 1, 4))),
            dma,
            dma((CHUNKS,)),
            dma((max(pairs - 1, 1), pairs)),
            dma,
            dma((4,)),
        ],
        compiler_params=pltpu.CompilerParams(collective_id=0, has_side_effects=True, vmem_limit_bytes=LIMIT),
    )(timestep, *args)
    return pl.pallas_call(
        project_out,
        out_shape=jax.ShapeDtypeStruct(latents.shape, bf16),
        in_specs=[vmem] * 3,
        out_specs=anywhere,
        scratch_shapes=[pltpu.VMEM((tok, width), bf16), dma((max(width // 512, 1),))],
        compiler_params=pltpu.CompilerParams(vmem_limit_bytes=8 * 2**20),
    )(att, wo, mod)


def solution(mesh):
    placed = (P("grp", "sp", None), P("grp"), P(), P("sp", "grp", None), P("sp", "grp", None))
    body = functools.partial(on_device, mesh.shape["grp"], mesh.shape["sp"])
    return jax.shard_map(
        body, mesh=mesh, in_specs=placed, out_specs=P("grp", "sp", None), check_vma=False
    )
```

```python
import functools
import math

import jax
import jax.numpy as jnp
from jax import lax
from jax.experimental import pallas as pl
from jax.experimental.pallas import tpu as pltpu
from jax.sharding import PartitionSpec as P

MESH = pl.DeviceIdType.MESH
CHUNKS = 4
LIMIT = 40 * 2**20


def embedding(timestep, freq):
    half_freq = freq // 2
    steps = lax.broadcasted_iota(jnp.int32, (8, half_freq), 1).astype(jnp.float32)
    angles = timestep.astype(jnp.float32) * jnp.exp(-math.log(10000.0) * steps / half_freq)
    return jnp.concatenate([jnp.cos(angles), jnp.sin(angles)], axis=1).astype(jnp.bfloat16)


def kernel(
    n_grp,
    n_sp,
    step_now,
    lat_hbm,
    wmod_hbm,
    wqkv_hbm,
    wout_hbm,
    att_mine,
    wo,
    mod,
    lat,
    wmod,
    normed,
    wq,
    q_buf,
    kv,
    att_send,
    att_far,
    loc_sem,
    q_s,
    o_s,
    lat_s,
    kv_s,
    at_s,
    wz_r,
    wx_r,
    wd_r,
    oz_r,
    ox_r,
    od_r,
    lat_r,
    kv_r,
    at_r,
    x_r,
    twin_in,
):
    g = lax.axis_index("grp")
    s = lax.axis_index("sp")
    core, chip = g % 2, g // 2
    chips = n_grp // 2
    pairs = n_sp // 2
    parity, pair = s % 2, s // 2
    tok, width = lat_hbm.shape[1], lat_hbm.shape[2]
    rows_q = wqkv_hbm.shape[1]
    rows_o = wout_hbm.shape[1]
    head = wqkv_hbm.shape[2] // 3
    sib = (chip * 2 + 1 - core, s)
    mate = (g, pair * 2 + 1 - parity)
    line = n_sp == 4
    inner = (parity + pair) % 2
    piece = tok // CHUNKS
    part_rows = tok - piece

    def at_chip(c):
        return ((chip + c) % chips * 2 + core, s)

    def at_pair(k, flip):
        return (g, (pair + k) % pairs * 2 + (parity + flip) % 2)

    def when_inner(body):
        pl.when(inner == 1)(body)

    def when_outer(body):
        pl.when(inner == 0)(body)

    def remote(src, dst, ssem, rsem, device):
        return pltpu.make_async_remote_copy(
            src_ref=src, dst_ref=dst, send_sem=ssem, recv_sem=rsem, device_id=device, device_id_type=MESH
        )

    def wq_rows(k, owner):
        return wq.at[pl.ds(pl.multiple_of(k * width + owner * rows_q, rows_q), rows_q), :]

    def wo_rows(par, k, owner):
        first = (par * pairs + k) * head + owner * rows_o
        return wo.at[pl.ds(pl.multiple_of(first, rows_o), rows_o), :]

    square = chips == 4
    near_x = chip // 2 * 2 + 1 - chip % 2
    near_y = (chip + 2) % 4
    corner = (near_x + 2) % 4
    to_x, to_y = (near_x * 2 + core, s), (near_y * 2 + core, s)

    def tell(sem, device):
        pl.semaphore_signal(sem, inc=1, device_id=device, device_id_type=MESH)

    barrier = pltpu.get_barrier_semaphore()
    peers = [sib] + ([to_x, to_y] if square else [at_chip(c) for c in range(1, chips)])
    if line:
        peers.append(mate)
    else:
        peers += [at_pair(k, f) for k in range(pairs) for f in range(2) if (k, f) != (0, 0)]
    for peer in peers:
        tell(barrier, peer)
    if line:

        @when_inner
        def _():
            tell(barrier, at_pair(1, 1))

    local = [
        pltpu.make_async_copy(wqkv_hbm.at[0], wq_rows(0, g), loc_sem.at[0]),
        pltpu.make_async_copy(wout_hbm.at[0], wo_rows(parity, 0, g), loc_sem.at[1]),
        pltpu.make_async_copy(lat_hbm.at[0], lat.at[0:tok, :], loc_sem.at[2]),
        pltpu.make_async_copy(wmod_hbm, wmod, loc_sem.at[3]),
    ]
    for copy in local:
        copy.start()
    local[0].wait()
    local[1].wait()
    if line:

        @when_inner
        def _():
            pl.semaphore_wait(barrier, len(peers) + 1)
            tell(twin_in, mate)
            tell(twin_in, at_pair(1, 1))

        @when_outer
        def _():
            pl.semaphore_wait(barrier, len(peers))

    else:
        pl.semaphore_wait(barrier, len(peers))

    def start(src, dst, ssem, rsem, device):
        remote(src, dst, ssem, rsem, device).start()

    def arrive(region, ssem, rsem):
        remote(region, region, ssem, rsem, sib).wait_recv()

    others = [near_x, near_y, corner] if square else [(chip + chips - c) % chips for c in range(1, chips)]

    def q_part(k, owner, half):
        size = rows_q // 2
        return wq.at[pl.ds(pl.multiple_of(k * width + owner * rows_q + half * size, size), size), :]

    def o_part(par, k, owner, half):
        first = (par * pairs + k) * head + owner * rows_o
        size = width // 2
        return wo.at[pl.ds(pl.multiple_of(first, rows_o), rows_o), half * size : (half + 1) * size]

    class Spread:
        def __init__(self, i, whole, part, ssem, xr, dr):
            self.i, self.whole, self.part = i, whole, part
            self.ssem, self.xr, self.dr = ssem, xr, dr

        def cross(self, region, slot, device):
            start(region, region, self.ssem, self.xr.at[self.i, slot], device)

        def land(self, region, slot):
            arrive(region, self.ssem, self.xr.at[self.i, slot])

        def to_sib(self, region):
            start(region, region, self.ssem, self.dr, sib)

        def begin(self):
            mine = self.whole(g)
            if square:
                self.cross(mine, 0, to_x)
                self.cross(mine, 1, to_y)
            else:
                for c in range(1, chips):
                    self.cross(mine, c - 1, at_chip(c))
            self.to_sib(mine)

        def relay(self):
            if square:
                for slot, device in ((0, to_y), (1, to_x)):
                    owner = others[slot] * 2 + core
                    self.land(self.whole(owner), slot)
                    self.cross(self.part(owner, slot), 2 + slot, device)
                    self.to_sib(self.whole(owner))
            else:
                for slot in range(chips - 1):
                    region = self.whole(others[slot] * 2 + core)
                    self.land(region, slot)
                    self.to_sib(region)

        def last(self):
            if square:
                owner = corner * 2 + core
                self.land(self.part(owner, 0), 2)
                self.land(self.part(owner, 1), 3)
                self.to_sib(self.whole(owner))

    def spread_q(k):
        whole, part = functools.partial(wq_rows, k), functools.partial(q_part, k)
        return Spread(k, whole, part, q_s, wx_r, wd_r.at[k])

    def spread_cols(k, slot, first, count):
        def cut(region):
            return region.at[:, first : first + count]

        def whole(owner):
            return cut(wq_rows(k, owner))

        def part(owner, half):
            return cut(q_part(k, owner, half))

        return Spread(slot, whole, part, q_s, wx_r, wd_r.at[slot])

    def finish_cols(k, slot, first, count):
        arrive(wq.at[k * width : k * width + width // 2, first : first + count], q_s, wd_r.at[slot])

    def finish_q(k):
        arrive(wq.at[k * width : k * width + width // 2, :], q_s, wd_r.at[k])

    def spread_o(k, flip):
        par = (parity + flip) % 2
        whole, part = functools.partial(wo_rows, par, k), functools.partial(o_part, par, k)
        return Spread(k * 2 + flip, whole, part, o_s, ox_r, od_r)

    far = [(k, f) for k in range(pairs) for f in range(2) if (k, f) != (0, 0)]
    all_q = [spread_q(k) for k in range(pairs)]
    near_o = spread_o(0, 0)

    def send_q():
        for k in range(1, pairs):
            start(wq_rows(0, g), wq_rows(k, g), q_s, wz_r.at[k], at_pair(k, 0))

    def pass_o(par, k_here, k_there, flip_there, device):
        start(wo_rows(par, k_here, g), wo_rows(par, k_there, g), o_s, oz_r.at[k_there * 2 + flip_there], device)

    def land_o(k, flip):
        arrive(wo_rows((parity + flip) % 2, k, g), o_s, oz_r.at[k * 2 + flip])

    def send_chunk(c):
        rows = c * piece
        start(lat.at[pl.ds(rows, piece), :], lat.at[pl.ds(tok + rows, piece), :], lat_s, lat_r.at[c], mate)

    def send_inner():
        start(lat.at[pl.ds(part_rows, piece), :], lat.at[pl.ds(2 * tok, piece), :], lat_s, x_r.at[0], at_pair(1, 1))

    step = min(512, width)

    def modulate():
        embed = embedding(step_now[0], wmod.shape[0])
        embed = jnp.concatenate([embed, embed], axis=0)
        local[3].wait()

        @pl.loop(0, 3 * width // step)
        def _(i):
            cols = pl.ds(pl.multiple_of(i * step, step), step)
            part = jnp.dot(embed, wmod[:, cols], preferred_element_type=jnp.float32)
            mod[:, cols] = part[:8]

    def normalize(first, count):
        block = 16

        @pl.loop(0, count // block)
        def _(i):
            rows = pl.ds(pl.multiple_of(first + i * block, block), block)
            values = lat[rows, :].astype(jnp.float32)
            center = jnp.mean(values, axis=-1, keepdims=True)
            values = values - center
            spread = jnp.mean(values * values, axis=-1, keepdims=True)
            scaled = values * lax.rsqrt(spread + 1e-06)
            shift = mod[0:1, 0:width]
            scale = mod[0:1, width : 2 * width]
            normed[rows, :] = (scaled * (1.0 + scale) + shift).astype(jnp.bfloat16)

    def land_chunk(c):
        arrive(lat.at[pl.ds(tok + c * piece, piece), :], lat_s, lat_r.at[c])

    def normalize_chunk(c):
        land_chunk(c)
        normalize(tok + c * piece, piece)

    def project(k, first, count):
        rows = pl.ds(first, count)
        weights = wq[k * width : (k + 1) * width, :]
        result = jnp.dot(normed[rows, :], weights, preferred_element_type=jnp.float32).astype(jnp.bfloat16)
        here = min(2 * tok - first, count)
        q_buf[k, pl.ds(first, here), :] = result[:here, :head]
        kv[0, k, pl.ds(first, here), :] = result[:here, head:]
        if here < count:
            q_buf[k, pl.ds(3 * tok - (count - here), count - here), :] = result[here:, :head]
            kv[1, k, pl.ds(2 * tok - (count - here), count - here), :] = result[here:, head:]

    def project_part(k, first, count, is_q):
        rows = pl.ds(first, count)
        weights = wq[k * width : (k + 1) * width, 0:head] if is_q else wq[k * width : (k + 1) * width, head:]
        result = jnp.dot(normed[rows, :], weights, preferred_element_type=jnp.float32).astype(jnp.bfloat16)
        here = min(2 * tok - first, count)
        if is_q:
            q_buf[k, pl.ds(first, here), :] = result[:here]
        else:
            kv[0, k, pl.ds(first, here), :] = result[:here]
        if here < count and is_q:
            q_buf[k, pl.ds(3 * tok - (count - here), count - here), :] = result[here:]
        elif here < count:
            kv[1, k, pl.ds(2 * tok - (count - here), count - here), :] = result[here:]

    def share_kv(k, first, count):
        rows = pl.ds(first, count)
        for d in range(1, pairs):
            there = (k + d) % pairs
            start(kv.at[0, k, rows, :], kv.at[d, there, rows, :], kv_s, kv_r.at[d - 1, there], at_pair(d, 0))

    def attention(k, first, count):
        total = pairs * 2 * tok
        keys = kv[:, k, :, :head].reshape(total, head)
        values = kv[:, k, :, head:].reshape(total, head)
        query = q_buf[k, pl.ds(first, count), :]
        scores = lax.dot_general(query, keys, (((1,), (1,)), ((), ())), preferred_element_type=jnp.float32)
        largest = jnp.max(scores, axis=1, keepdims=True)
        weights = jnp.exp((scores - largest) * (1.0 / math.sqrt(head)))
        mixed = jnp.dot(weights.astype(jnp.bfloat16), values, preferred_element_type=jnp.float32)
        return (mixed / jnp.sum(weights, axis=1, keepdims=True)).astype(jnp.bfloat16)

    def send_att(k):
        start(att_send.at[k], att_mine.at[parity * pairs + k], at_s, at_r, mate)

    def drain(region, ssem):
        remote(region, region, ssem, at_r, sib).wait_send()

    spread_sends = 7 if square else 2 * chips - 1

    def drain_o(passed):
        drain(wq.at[0 : (n_sp * spread_sends + passed) * rows_o * width // (3 * head), :], o_s)

    def general():
        far_o = [spread_o(k, f) for k, f in far]

        def send_o(n):
            for k, f in far[n : n + 1]:
                pass_o(parity, 0, k, f, at_pair(k, f))

        def take_o(n):
            land_o(*far[n])
            far_o[n].begin()

        all_q[0].begin()
        near_o.begin()
        send_q()
        local[2].wait()
        send_chunk(0)
        modulate()
        normalize(0, tok)
        all_q[0].relay()
        near_o.relay()
        send_chunk(1)
        for k in range(1, pairs):
            arrive(wq_rows(k, g), q_s, wz_r.at[k])
            all_q[k].begin()
        send_o(0)
        send_chunk(2)
        send_o(1)
        send_chunk(3)
        for n in range(2, len(far)):
            send_o(n)
        all_q[0].last()
        finish_q(0)
        project(0, 0, tok)
        share_kv(0, 0, tok)
        near_o.last()
        for k in range(1, pairs):
            all_q[k].relay()
        normalize_chunk(0)
        for k in range(1, pairs):
            all_q[k].last()
            finish_q(k)
            project(k, 0, tok)
            share_kv(k, 0, tok)
        take_o(0)
        take_o(1)
        for c in range(1, CHUNKS):
            normalize_chunk(c)
        for k in range(pairs):
            project(k, tok, tok)
            share_kv(k, tok, tok)
        far_o[0].relay()
        for n in range(2, len(far)):
            take_o(n)
        far_o[1].relay()
        far_o[0].last()
        for spread in far_o[2:]:
            spread.relay()
        far_o[1].last()
        for k in range(pairs):
            for d in range(1, pairs):
                arrive(kv.at[d, k], kv_s, kv_r.at[d - 1, k])
            att_send[k] = attention(k, tok, tok)
            send_att(k)
            att_mine[parity * pairs + k] = attention(k, 0, tok)
        for spread in far_o[2:]:
            spread.last()
        arrive(wo.at[0 : n_sp * head // 2, :], o_s, od_r)
        arrive(att_send, at_s, at_r)
        drain_o(n_sp - 1)
        for d in range(1, pairs):
            drain(kv.at[0], kv_s)
        drain(att_send, at_s)

    def along_line():
        far_a, far_b, far_c = spread_o(0, 1), spread_o(1, inner), spread_o(1, 1 - inner)
        cols = {"kv": (1, head, 2 * head), "q": (2, 0, head)}
        other = {name: spread_cols(1, *cut) for name, cut in cols.items()}
        late = tok + 2 * piece

        def send_other(name):
            slot, first, count = cols[name]
            source, target = wq_rows(0, g), wq_rows(1, g)
            width_of = slice(first, first + count)
            start(source.at[:, width_of], target.at[:, width_of], q_s, wz_r.at[slot], at_pair(1, 0))

        def take_other(name):
            slot, first, count = cols[name]
            arrive(wq_rows(1, g).at[:, first : first + count], q_s, wz_r.at[slot])
            other[name].begin()

        all_q[0].begin()
        near_o.begin()
        local[2].wait()

        @when_inner
        def _():
            pl.semaphore_wait(twin_in, 1)
            send_other("kv")

        @when_outer
        def _():
            send_chunk(0)
            pl.semaphore_wait(twin_in, 1)
            send_other("kv")
            pass_o(parity, 0, 0, 1, mate)

        modulate()
        normalize(0, tok)

        @when_inner
        def _():
            send_chunk(0)

        all_q[0].relay()
        send_other("q")

        @when_inner
        def _():
            pass_o(parity, 0, 0, 1, mate)
            pass_o(parity, 0, 1, 1, at_pair(1, 1))

        @when_outer
        def _():
            for c in range(1, CHUNKS):
                send_chunk(c)

        take_other("kv")
        near_o.relay()

        @when_inner
        def _():
            send_chunk(1)
            send_chunk(2)
            land_o(0, 1)
            pass_o(1 - parity, 0, 1, 0, at_pair(1, 1))

        normalize_chunk(0)
        all_q[0].last()
        finish_q(0)
        project(0, 0, tok)

        @when_outer
        def _():
            share_kv(0, 0, tok)

        @when_inner
        def _():
            land_o(1, 1)
            pass_o(1 - parity, 1, 1, 0, mate)

        take_other("q")
        near_o.last()
        other["kv"].relay()

        @when_inner
        def _():
            land_o(1, 0)
            pass_o(parity, 1, 1, 1, mate)
            send_inner()

        @when_outer
        def _():
            land_o(0, 1)

        far_a.begin()
        normalize_chunk(1)
        project(0, tok, 2 * piece)

        @when_outer
        def _():
            share_kv(0, tok, 2 * piece)

        other["q"].relay()

        @when_inner
        def _():
            far_b.begin()
            far_c.begin()
            normalize_chunk(2)
            share_kv(0, 0, late)

        other["kv"].last()
        finish_cols(1, *cols["kv"])
        project_part(1, 0, late, False)

        share_kv(1, 0, late)

        @when_outer
        def _():
            land_o(1, 0)
            far_b.begin()

        far_a.relay()
        other["q"].last()
        finish_cols(1, *cols["q"])

        @when_inner
        def _():
            land_chunk(3)
            arrive(lat.at[pl.ds(2 * tok, piece), :], lat_s, x_r.at[0])
            normalize(late + piece, 2 * piece)
            far_b.relay()
            rows = pl.ds(2 * tok - piece, piece)

            def pass_kv(k):
                start(kv.at[1, k, rows, :], kv.at[0, 1 - k, rows, :], kv_s, x_r.at[2 - k], at_pair(1, 0))
                share_kv(k, late, 2 * piece)

            project(0, late, 3 * piece)
            pass_kv(0)
            project_part(1, late, 3 * piece, False)
            pass_kv(1)
            far_c.relay()
            project_part(1, 0, 2 * tok + piece, True)

        @when_outer
        def _():
            normalize_chunk(2)
            rows, there = pl.ds(tok, part_rows), pl.ds(2 * tok, part_rows)

            def pass_query(k):
                start(q_buf.at[k, rows, :], q_buf.at[1 - k, there, :], at_s, x_r.at[2 - k], at_pair(1, 0))

            project(0, late, piece)
            share_kv(0, late, piece)
            pass_query(0)
            project_part(1, late, piece, False)
            share_kv(1, late, piece)
            project_part(1, 0, late + piece, True)
            pass_query(1)
            land_o(1, 1)
            far_c.begin()
            far_b.relay()
            far_c.relay()

        far_a.last()
        far_b.last()
        far_c.last()

        @when_inner
        def _():
            for k in range(pairs):
                arrive(kv.at[1, k, pl.ds(0, tok + part_rows), :], kv_s, kv_r.at[0, k])
                arrive(q_buf.at[k, pl.ds(2 * tok, part_rows), :], at_s, x_r.at[1 + k])
            for k in range(pairs):
                result = attention(k, tok, 2 * tok)
                att_send[k] = result[:tok]
                att_far[k] = result[tok:]
            for k in range(pairs):
                send_att(k)
                start(att_far.at[k], att_mine.at[parity * pairs + 1 - k], at_s, at_r, at_pair(1, 1))

        @when_outer
        def _():
            for k in range(pairs):
                arrive(kv.at[1, k], kv_s, kv_r.at[0, k])
                arrive(kv.at[0, k, pl.ds(2 * tok - piece, piece), :], kv_s, x_r.at[1 + k])

        for k in range(pairs):
            att_mine[parity * pairs + k] = attention(k, 0, tok)
        arrive(wo.at[0 : n_sp * head // 2, :], o_s, od_r)
        arrive(att_send, at_s, at_r)

        @when_inner
        def _():
            drain_o(5)
            drain(lat.at[0 : pairs * (2 * tok + piece) * 2 * head // width, :], kv_s)
            drain(q_buf.at[:, 0 : 2 * tok, :], at_s)

        @when_outer
        def _():
            drain_o(1)
            drain(kv.at[0, :, pl.ds(0, tok + part_rows), :], kv_s)
            drain(q_buf.at[:, 0:part_rows, :], at_s)

    if line:
        along_line()
    else:
        general()
    drain(wq.at[0 : (pairs * spread_sends + pairs - 1) * rows_q, :], q_s)
    drain(lat.at[0:tok, :], lat_s)


def project_out(att, wo, mod, out_hbm, out_buf, sems):
    width = wo.shape[1]
    step = width // sems.shape[0]
    mixed = jnp.concatenate([att[i] for i in range(att.shape[0])], axis=1)
    outs = []
    for i in range(sems.shape[0]):
        cols = slice(i * step, (i + 1) * step)
        total = jnp.dot(mixed, wo[:, cols], preferred_element_type=jnp.float32)
        gate = mod[0:1, 2 * width + i * step : 2 * width + (i + 1) * step]
        out_buf[:, cols] = (gate * total).astype(jnp.bfloat16)
        outs.append(pltpu.make_async_copy(out_buf.at[:, cols], out_hbm.at[0, :, cols], sems.at[i]))
        outs[i].start()
    for copy in outs:
        copy.wait()


def on_device(n_grp, n_sp, latents, timestep, w_mod, w_qkv, w_out):
    _, tok, width = latents.shape
    head = w_qkv.shape[2] // 3
    pairs, chips = n_sp // 2, n_grp // 2
    dma = pltpu.SemaphoreType.DMA
    bf16 = jnp.bfloat16
    anywhere = pl.BlockSpec(memory_space=pl.ANY)
    vmem = pl.BlockSpec(memory_space=pltpu.VMEM)
    args = [pltpu.with_memory_space_constraint(a, pltpu.HBM) for a in (latents, w_mod, w_qkv, w_out)]
    att, wo, mod = pl.pallas_call(
        functools.partial(kernel, n_grp, n_sp),
        out_shape=[
            pltpu.VMEM((n_sp, tok, head), bf16),
            pltpu.VMEM((n_sp * head, width), bf16),
            pltpu.VMEM((8, w_mod.shape[1]), jnp.float32),
        ],
        in_specs=[pl.BlockSpec(memory_space=pltpu.SMEM)] + [anywhere] * 4,
        out_specs=[vmem] * 3,
        scratch_shapes=[
            pltpu.VMEM((2 * tok + tok // CHUNKS, width), bf16),
            pltpu.VMEM(w_mod.shape, bf16),
            pltpu.VMEM((2 * tok + tok // CHUNKS, width), bf16),
            pltpu.VMEM((pairs * width, 3 * head), bf16),
            pltpu.VMEM((pairs, 3 * tok, head), bf16),
            pltpu.VMEM((pairs, pairs, 2 * tok, 2 * head), bf16),
            pltpu.VMEM((pairs, tok, head), bf16),
            pltpu.VMEM((pairs, tok, head), bf16),
            dma((4,)),
            dma,
            dma,
            dma,
            dma,
            dma,
            dma((max(pairs, 3),)),
            dma((max(pairs, 3), max(chips - 1, 4))),
            dma((max(pairs, 3),)),
            dma((n_sp,)),
            dma((n_sp, max(chips - 1, 4))),
            dma,
            dma((CHUNKS,)),
            dma((max(pairs - 1, 1), pairs)),
            dma,
            dma((4,)),
            pltpu.SemaphoreType.REGULAR,
        ],
        compiler_params=pltpu.CompilerParams(collective_id=0, has_side_effects=True, vmem_limit_bytes=LIMIT),
    )(timestep, *args)
    return pl.pallas_call(
        project_out,
        out_shape=jax.ShapeDtypeStruct(latents.shape, bf16),
        in_specs=[vmem] * 3,
        out_specs=anywhere,
        scratch_shapes=[pltpu.VMEM((tok, width), bf16), dma((max(width // 512, 1),))],
        compiler_params=pltpu.CompilerParams(vmem_limit_bytes=8 * 2**20),
    )(att, wo, mod)


def solution(mesh):
    placed = (P("grp", "sp", None), P("grp"), P(), P("sp", "grp", None), P("sp", "grp", None))
    body = functools.partial(on_device, mesh.shape["grp"], mesh.shape["sp"])
    return jax.shard_map(
        body, mesh=mesh, in_specs=placed, out_specs=P("grp", "sp", None), check_vma=False
    )
```
